256 devices in a mesh: dp: 8 (over x, core), vocab: 32 (over z, y).
Axes of the slice: x: 4, y: 4, z: 8, core: 2. Of those that a mesh axis runs over, the one named last changes fastest.
Arguments:
- hidden: bfloat16 [1024, 8192], P('dp'), may hold values from -600 to 600
- out_weight: bfloat16 [8192, 98304], P('dp', 'vocab'), may hold values from -0.5 to 0.5
- targets: int32 [1024], P('dp'), may hold values from 0 to 98303
- segment: int32 [1024], P('dp'), may hold values from 0 to 31, never falling along the last dimension, each value on 1 to 64 neighbouring positions
- loss_mask: int32 [1024], P('dp'), may hold values 0 or 1
- outside_count: int32 [32], replicated, may hold values from 0 to 3
Outputs:
- token_loss: float32 [1024], P('dp')
- sample_loss: float32 [32], replicated
The draws below stay inside these ranges and needn't reach their ends.
All inputs are finite; a program needn't handle non-finite values. No bound on the sum of `loss_mask` on one device may be relied on, other than what follows from the above.
Results may differ from the reference program's by a relative error of at most 0.0003.
Values may be sent and summed in bfloat16 or wider, within the bound.
A program may use at most 64 MiB of HBM per device.

```python
import math
import jax
import jax.numpy as jnp
import numpy as np
from jax import lax

D = 8192
V = 98304
TOKENS = 1024
SAMPLES = 32
SEG_MOST = 64


def weight_full(key):
    base = jax.random.normal(jax.random.fold_in(key, 7), (D, V), jnp.float32) * D ** (-0.5)
    return base


def draw_out_weight(key, part):
    return weight_full(key).astype(jnp.bfloat16)


def draw_hidden(key, part):
    states = jax.random.normal(jax.random.fold_in(key, 21), (TOKENS, D), jnp.float32) * 3.0
    return states.astype(jnp.bfloat16)


def set_ends(entries, key, smallest, top_value):
    index_at = [jax.random.randint(jax.random.fold_in(key, axis), (), 0, length) for axis, length in enumerate(entries.shape)]
    longest = entries.shape.index(max(entries.shape))
    neighbour = index_at[:longest] + [(index_at[longest] + 1) % entries.shape[longest]] + index_at[longest + 1:]
    return entries.at[tuple(index_at)].set(smallest).at[tuple(neighbour)].set(top_value)


def ranked_wide(stream_key, shape, number_of, slope):
    portions = [min(1 << octave, number_of + 1 - (1 << octave)) * (1 << 20) // math.isqrt((1 << octave) ** slope) + 1 for octave in range((number_of + 1).bit_length()) if 1 << octave <= number_of]
    spread = 1 + sum(portions) // (1 << 30)
    grid = np.cumsum(np.array([max(1, weight // spread) for weight in portions]))
    lot = jax.random.randint(jax.random.fold_in(stream_key, 1), shape, 0, int(grid[len(portions) - 1]))
    start = jnp.left_shift(1, jnp.searchsorted(jnp.asarray(grid, jnp.int32), lot, side="right").astype(jnp.int32))
    standing = start - 1 + jax.random.randint(jax.random.fold_in(stream_key, 4), shape, 0, 1 << 30) % jnp.minimum(start, number_of + 1 - start)
    return jax.random.permutation(jax.random.fold_in(stream_key, 2), number_of)[standing].astype(jnp.int32)


def length_profile(amount, total, reach, skew):
    weights = [(1 << 20) // math.isqrt(standing ** skew) + 1 for standing in range(2, amount + 1)]
    surplus, holding = total - reach - (amount - 1), [1] * (amount - 1)
    while surplus > 0:
        candidates = [i for i in range(amount - 1) if holding[i] < reach]
        pool, left = sum([weights[i] for i in candidates]), surplus
        for i in candidates:
            extra = min(reach - holding[i], max(1, left * weights[i] // pool), surplus)
            holding[i] = holding[i] + extra
            surplus = surplus - extra
    return np.array([reach] + holding)


def uneven(rng, number_of, total, reach, skew):
    if number_of == 2:
        one = jax.random.randint(rng, (), max(1, total - reach), min(reach, total - 1) + 1)
        return jnp.stack([one, total - one])
    lengths = jnp.asarray(length_profile(number_of, total, reach, skew), jnp.int32)
    couples = (number_of - 1) // 2
    donor, receiver = lengths[1:1 + 2 * couples:2], lengths[2:2 + 2 * couples:2]
    slack = jnp.minimum(donor - 1, reach - receiver)
    moved = jax.random.randint(jax.random.fold_in(rng, 1), (couples,), 0, 1 << 20) % (slack + 1)
    lengths = lengths.at[1:1 + 2 * couples:2].set(donor - moved).at[2:2 + 2 * couples:2].set(receiver + moved)
    return lengths[jax.random.permutation(jax.random.fold_in(rng, 2), number_of)]


def setup_inputs(seed: int = 0) -> dict:
    seeds = jax.random.split(jax.random.key(seed), 7)
    return {
        "hidden": draw_hidden(jax.random.fold_in(seeds[6], 71), 0),
        "out_weight": draw_out_weight(jax.random.fold_in(seeds[6], 71), 0),
        "targets": set_ends(ranked_wide(seeds[2], (TOKENS,), V, 2), jax.random.fold_in(seeds[2], 3), 0, V - 1).astype(jnp.int32),
        "segment": jnp.searchsorted(jnp.cumsum(uneven(seeds[3], SAMPLES, TOKENS, SEG_MOST, 2)), jnp.arange(TOKENS), side="right").astype(jnp.int32),
        "loss_mask": set_ends((jax.random.randint(seeds[4], (TOKENS,), 0, 4) < 3).astype(jnp.int32), jax.random.fold_in(seeds[4], 1), 0, 1),
        "outside_count": set_ends(jax.random.randint(seeds[5], (SAMPLES,), 0, 4), jax.random.fold_in(seeds[5], 1), 0, 3).astype(jnp.int32),
    }


def reference(hidden, out_weight, targets, segment, loss_mask, outside_count):
    block_rows = math.gcd(TOKENS, 256)
    block_count = TOKENS // block_rows
    hidden_blocks = hidden.reshape(block_count, block_rows, D)
    target_blocks = targets.reshape(block_count, block_rows)

    def one_block(pair):
        rows_block, target_block = pair
        logits = jnp.dot(rows_block, out_weight, preferred_element_type=jnp.float32)
        largest = jnp.max(logits, axis=1)
        lse = largest + jnp.log(jnp.sum(jnp.exp(logits - largest[:, None]), axis=1))
        picked = jnp.take_along_axis(logits, target_block[:, None].astype(jnp.int32), axis=1)[:, 0]
        return lse - picked

    token_loss = lax.map(one_block, (hidden_blocks, target_blocks)).reshape(TOKENS)
    onehot = (segment[:, None] == jnp.arange(SAMPLES, dtype=jnp.int32)[None, :]).astype(jnp.float32)
    weights = loss_mask.astype(jnp.float32)
    loss_sum = jnp.dot(token_loss * weights, onehot, precision=lax.Precision.HIGHEST)
    count = jnp.dot(weights, onehot, precision=lax.Precision.HIGHEST)
    denom = jnp.maximum(count + outside_count.astype(jnp.float32), 1.0)
    return token_loss, loss_sum / denom
```

```python
import functools

import jax
import jax.numpy as jnp
from jax import lax
from jax.experimental import pallas as pl
from jax.experimental.pallas import tpu as pltpu
from jax.sharding import PartitionSpec as P

CORES = 2
NY = 4
SAMPLES_MOST = 128
LOW = -3.0e38


def kernel(
    nx, nz, chunks,
    hid, w, tgt, seg, msk, outside,
    o_tok, o_samp,
    feats, weights, meta_out, meta, sent, got, logits,
    st1_out, st1, st2_out, st2, st3_out, st3,
    loc_sem, w_send, w_recv, own_send, own_recv, meta_send, meta_recv,
    hx_send, hx_recv, hy_send, hy_recv, hd_send, hd_recv,
    ring_send, ring_recv,
    s1_send, s1_recv, s2_send, s2_recv, s3_send, s3_recv,
):
    dp = lax.axis_index("dp")
    vocab = lax.axis_index("vocab")
    x, c = dp // CORES, dp % CORES
    z, y = vocab // NY, vocab % NY
    rows = hid.shape[0]
    depth = w.shape[0]
    chip_feats = CORES * depth
    piece = chip_feats // NY
    width = weights.shape[2]
    half_cols = w.shape[1] // CORES

    def dev(xx, cc, zz, yy):
        return (xx * CORES + cc, zz * NY + yy)

    def remote(src, dst, send, recv, to):
        return pltpu.make_async_remote_copy(
            src_ref=src, dst_ref=dst, send_sem=send, recv_sem=recv,
            device_id=to, device_id_type=pl.DeviceIdType.MESH,
        )

    partner = dev(x, 1 - c, z, y)
    y_up, y_down = dev(x, c, z, (y + 1) % NY), dev(x, c, z, (y + NY - 1) % NY)
    x_up, x_down = dev((x + 1) % nx, c, z, y), dev((x + nx - 1) % nx, c, z, y)
    slot1 = y * CORES + c
    n1 = NY * CORES

    def peer1(j):
        s = (slot1 + j) % n1
        return s, dev(x, s % CORES, z, s // CORES)

    def peer2(j):
        s = (z + j) % nz
        return s, dev(x, c, s, y)

    def peer3(j):
        s = (x + j) % nx
        return s, dev(s, c, z, y)

    my_rows = pl.ds(pl.multiple_of(c * rows, rows), rows)
    his_rows = pl.ds(pl.multiple_of((1 - c) * rows, rows), rows)

    meta_out[...] = jnp.zeros_like(meta_out)
    meta_out[0:1, :] = tgt[...]
    meta_out[1:2, :] = seg[...]
    meta_out[2:3, :] = msk[...]
    meta[c] = meta_out[...]
    own_cols = pl.ds(pl.multiple_of(x * chip_feats, 128), chip_feats)
    local_h = pltpu.make_async_copy(
        hid.at[:, own_cols], feats.at[x, my_rows, :], loc_sem.at[0]
    )
    local_h.start()
    my_depth = pl.ds(pl.multiple_of(c * depth, depth), depth)
    his_depth = pl.ds(pl.multiple_of((1 - c) * depth, depth), depth)
    local_w = []
    for j in range(2 * chunks):
        cols = pl.ds(pl.multiple_of(c * half_cols + j * width, 128), width)
        copy = pltpu.make_async_copy(w.at[:, cols], weights.at[j, my_depth, :], loc_sem.at[1 + j])
        copy.start()
        local_w.append(copy)

    barrier = pltpu.get_barrier_semaphore()
    peers = [peer1(j)[1] for j in range(1, n1)]
    peers += [peer2(j)[1] for j in range(1, nz)]
    peers += [peer3(j)[1] for j in range(1, nx)]
    for p in peers:
        pl.semaphore_signal(barrier, inc=1, device_id=p, device_id_type=pl.DeviceIdType.MESH)
    pl.semaphore_wait(barrier, len(peers))

    order = [2, 1, 3]
    y_cols = pl.ds(pl.multiple_of(y * piece, 128), piece)

    def x_copy(d):
        to = (x + d) % nx
        cols = pl.ds(pl.multiple_of(to * chip_feats + y * piece, 128), piece)
        return remote(
            hid.at[:, cols], feats.at[x, my_rows, y_cols],
            hx_send.at[d - 1], hx_recv.at[d - 1], dev(to, c, z, y),
        )

    def w_copy(j):
        cols = pl.ds(pl.multiple_of((1 - c) * half_cols + j * width, 128), width)
        return remote(w.at[:, cols], weights.at[j, my_depth, :], w_send.at[j], w_recv.at[j], partner)

    for d in order:
        x_copy(d).start()
    for j in range(2 * chunks):
        w_copy(j).start()
    own_copy = remote(hid.at[:, own_cols], feats.at[x, my_rows, :], own_send, own_recv, partner)
    own_copy.start()
    meta_copy = remote(meta_out, meta.at[c], meta_send, meta_recv, partner)
    meta_copy.start()

    def place(s, which, part):
        cols = pl.ds(pl.multiple_of(((y + which) % NY) * piece, 128), piece)
        if part is None:
            return feats.at[s, my_rows, cols]
        half = rows // 2
        at = pl.ds(pl.multiple_of(c * rows + part * half, half), half)
        return feats.at[s, at, cols]

    def y_copy(d, s, i):
        which, part, to = [(0, None, y_up), (0, None, y_down), (NY - 1, 0, y_up), (1, 1, y_down)][i]
        ref = place(s, which, part)
        return remote(ref, ref, hy_send.at[d - 1, i], hy_recv.at[d - 1, i], to)

    def y_arrival(d, s, i):
        which, part = [(NY - 1, None), (1, None), (2, 0), (2, 1)][i]
        ref = place(s, which, part)
        return remote(ref, ref, hy_send.at[d - 1, i], hy_recv.at[d - 1, i], y_up)

    def d_copy(d, s, i):
        which, part = [(0, None), (NY - 1, None), (1, None), (2, 0), (2, 1)][i]
        ref = place(s, which, part)
        return remote(ref, ref, hd_send.at[d - 1, i], hd_recv.at[d - 1, i], partner)

    def source(d):
        return (x + nx - d) % nx

    def begin(d):
        s = source(d)
        x_copy(d).wait_recv()
        y_copy(d, s, 0).start()
        y_copy(d, s, 1).start()
        d_copy(d, s, 0).start()

    def finish(d):
        s = source(d)
        y_arrival(d, s, 0).wait_recv()
        y_copy(d, s, 2).start()
        d_copy(d, s, 1).start()
        y_arrival(d, s, 1).wait_recv()
        y_copy(d, s, 3).start()
        d_copy(d, s, 2).start()
        for i in (2, 3):
            y_arrival(d, s, i).wait_recv()
            d_copy(d, s, i + 1).start()
        for i in range(5):
            d_copy(d, s, i).wait_recv()

    def close(d):
        s = source(d)
        x_copy(d).wait_send()
        for i in range(4):
            y_copy(d, s, i).wait_send()
        for i in range(5):
            d_copy(d, s, i).wait_send()

    def part(block, j):
        return jnp.dot(feats[block], weights[j], preferred_element_type=jnp.float32)

    targets = (x_down, x_up, x_up, x_down, x_down, x_up)

    def message(i, k):
        return remote(sent.at[i, k], got.at[i, k], ring_send.at[i, k], ring_recv.at[i, k], targets[i])

    def put(i, k, value):
        sent[i, k] = value
        message(i, k).start()

    def take(i, k):
        message(i, k).wait_recv()
        return got[i, k]

    up, down, far = (x + 1) % nx, (x + nx - 1) % nx, (x + 2) % nx

    for d in order:
        begin(d)
    finish(2)
    for copy in local_w:
        copy.wait()
    for j in range(2 * chunks):
        w_copy(j).wait_recv()

    def first(k, carry):
        put(0, k, part(far, k))
        put(1, k, part(far, chunks + k))
        return carry

    lax.fori_loop(0, chunks, first, 0)
    finish(1)
    finish(3)

    def direct(k, carry):
        put(2, k, part(up, k))
        put(3, k, part(down, chunks + k))
        return carry

    lax.fori_loop(0, chunks, direct, 0)

    def relay(k, carry):
        own_a = part(down, k)
        put(4, k, own_a + take(0, k))
        own_b = part(up, chunks + k)
        put(5, k, own_b + take(1, k))
        return carry

    lax.fori_loop(0, chunks, relay, 0)

    local_h.wait()
    own_copy.wait_recv()
    meta_copy.wait_recv()

    def own(k, carry):
        logits[k] = part(x, k) + take(2, k)
        logits[chunks + k] = part(x, chunks + k) + take(3, k)
        return carry

    lax.fori_loop(0, chunks, own, 0)

    eye = lax.broadcasted_iota(jnp.int32, (rows, rows), 0) == lax.broadcasted_iota(jnp.int32, (rows, rows), 1)

    def to_column(row):
        return jnp.sum(jnp.where(eye, jnp.broadcast_to(row, (rows, rows)), 0.0), axis=1, keepdims=True)

    def to_row(column):
        return jnp.sum(jnp.where(eye, jnp.broadcast_to(column, (rows, rows)), 0.0), axis=0, keepdims=True)

    base = vocab * w.shape[1] + c * half_cols
    target_column = jnp.concatenate(
        [to_column((meta[i, 0:1, :] - base).astype(jnp.float32)) for i in range(CORES)], axis=0
    ).astype(jnp.int32)
    lane = lax.broadcasted_iota(jnp.int32, (CORES * rows, width), 1)

    def stats(j, value, carry):
        largest, total, picked = carry
        new = jnp.maximum(largest, jnp.max(value, axis=1, keepdims=True))
        total = total * jnp.exp(largest - new) + jnp.sum(jnp.exp(value - new), axis=1, keepdims=True)
        hit = lane == target_column - j * width
        picked = picked + jnp.sum(jnp.where(hit, value, 0.0), axis=1, keepdims=True)
        return new, total, picked

    def last(k, carry):
        carry = stats(k, logits[k] + take(4, k), carry)
        return stats(chunks + k, logits[chunks + k] + take(5, k), carry)

    column = (CORES * rows, 1)
    start = (jnp.full(column, LOW, jnp.float32), jnp.zeros(column, jnp.float32), jnp.zeros(column, jnp.float32))
    found = lax.fori_loop(0, chunks, last, start)

    for kind, value in enumerate(found):
        for i in range(CORES):
            st1_out[2 * kind + i : 2 * kind + i + 1, :] = to_row(value[i * rows : (i + 1) * rows])
    st1_out[6:8, :] = jnp.zeros((2, rows), jnp.float32)

    def exchange(n, me, peer, out, buf, send, recv):
        buf[me] = out[...]
        copies = []
        for j in range(1, n):
            _, to = peer(j)
            copy = remote(out, buf.at[me], send.at[j], recv.at[me], to)
            copy.start()
            copies.append(copy)
        for j in range(1, n):
            s, to = peer(j)
            remote(out, buf.at[s], send.at[j], recv.at[s], to).wait_recv()
        return copies

    def merged(n, buf):
        largest = buf[0, 0:2, :]
        for i in range(1, n):
            largest = jnp.maximum(largest, buf[i, 0:2, :])
        total, picked = jnp.zeros_like(largest), jnp.zeros_like(largest)
        for i in range(n):
            total = total + buf[i, 2:4, :] * jnp.exp(buf[i, 0:2, :] - largest)
            picked = picked + buf[i, 4:6, :]
        return largest, total, picked

    pending = exchange(n1, slot1, peer1, st1_out, st1, s1_send, s1_recv)
    for kind, value in enumerate(merged(n1, st1)):
        st2_out[2 * kind : 2 * kind + 2, :] = value
    st2_out[6:8, :] = jnp.zeros((2, rows), jnp.float32)
    pending += exchange(nz, z, peer2, st2_out, st2, s2_send, s2_recv)
    largest, total, picked = merged(nz, st2)
    loss = largest + jnp.log(total) - picked
    o_tok[...] = jnp.where(c == 0, loss[0:1], loss[1:2])

    ids = lax.broadcasted_iota(jnp.int32, (SAMPLES_MOST, rows), 0)
    sums, counts = jnp.zeros((SAMPLES_MOST, 1), jnp.float32), jnp.zeros((SAMPLES_MOST, 1), jnp.float32)
    for i in range(CORES):
        member = ids == meta[i, 1:2, :]
        weight = meta[i, 2:3, :].astype(jnp.float32)
        sums = sums + jnp.sum(jnp.where(member, weight * loss[i : i + 1], 0.0), axis=1, keepdims=True)
        counts = counts + jnp.sum(jnp.where(member, weight, 0.0), axis=1, keepdims=True)
    st3_out[...] = jnp.zeros_like(st3_out)
    st3_out[0:1, :] = to_row(sums)
    st3_out[1:2, :] = to_row(counts)
    pending += exchange(nx, x, peer3, st3_out, st3, s3_send, s3_recv)
    everything = st3[0]
    for i in range(1, nx):
        everything = everything + st3[i]
    samples = outside.shape[1]
    denom = jnp.maximum(everything[1:2, :samples] + outside[...].astype(jnp.float32), 1.0)
    o_samp[...] = everything[0:1, :samples] / denom

    for copy in pending:
        copy.wait_send()
    for d in order:
        close(d)
    for j in range(2 * chunks):
        w_copy(j).wait_send()
    own_copy.wait_send()
    meta_copy.wait_send()

    def drain(k, carry):
        for i in range(6):
            message(i, k).wait_send()
        return carry

    lax.fori_loop(0, chunks, drain, 0)


def body(nx, nz, hidden, out_weight, targets, segment, loss_mask, outside_count):
    rows, depth = hidden.shape[0], out_weight.shape[0]
    half_cols = out_weight.shape[1] // CORES
    width = min(256, half_cols // 2)
    chunks = half_cols // 2 // width
    f32, dma = jnp.float32, pltpu.SemaphoreType.DMA
    samples = outside_count.shape[0]
    n1 = NY * CORES
    vmem = pl.BlockSpec(memory_space=pltpu.VMEM)
    far = pl.BlockSpec(memory_space=pl.ANY)
    tok, samp = pl.pallas_call(
        functools.partial(kernel, nx, nz, chunks),
        out_shape=(
            jax.ShapeDtypeStruct((1, rows), f32),
            jax.ShapeDtypeStruct((1, samples), f32),
        ),
        in_specs=[far, far, vmem, vmem, vmem, vmem],
        out_specs=(vmem, vmem),
        scratch_shapes=[
            pltpu.VMEM((nx, CORES * rows, CORES * depth), jnp.bfloat16),
            pltpu.VMEM((2 * chunks, CORES * depth, width), jnp.bfloat16),
            pltpu.VMEM((8, rows), jnp.int32),
            pltpu.VMEM((CORES, 8, rows), jnp.int32),
            pltpu.VMEM((6, chunks, CORES * rows, width), f32),
            pltpu.VMEM((6, chunks, CORES * rows, width), f32),
            pltpu.VMEM((2 * chunks, CORES * rows, width), f32),
            pltpu.VMEM((8, rows), f32),
            pltpu.VMEM((n1, 8, rows), f32),
            pltpu.VMEM((8, rows), f32),
            pltpu.VMEM((nz, 8, rows), f32),
            pltpu.VMEM((8, SAMPLES_MOST), f32),
            pltpu.VMEM((nx, 8, SAMPLES_MOST), f32),
            dma((1 + 2 * chunks,)),
            dma((2 * chunks,)), dma((2 * chunks,)),
            dma, dma, dma, dma,
            dma((nx - 1,)), dma((nx - 1,)),
            dma((nx - 1, 4)), dma((nx - 1, 4)),
            dma((nx - 1, 5)), dma((nx - 1, 5)),
            dma((6, chunks)), dma((6, chunks)),
            dma((n1,)), dma((n1,)),
            dma((nz,)), dma((nz,)),
            dma((nx,)), dma((nx,)),
        ],
        compiler_params=pltpu.CompilerParams(collective_id=0, has_side_effects=True),
    )(
        hidden, out_weight, targets[None], segment[None], loss_mask[None], outside_count[None]
    )
    return tok.reshape(rows), samp.reshape(samples)


def solution(mesh):
    nx = mesh.shape["dp"] // CORES
    nz = mesh.shape["vocab"] // NY
    return jax.shard_map(
        functools.partial(body, nx, nz),
        mesh=mesh,
        in_specs=(P("dp", None), P("dp", "vocab"), P("dp"), P("dp"), P("dp"), P()),
        out_specs=(P("dp"), P()),
        check_vma=False,
    )
```

```python
import functools

import jax
import jax.numpy as jnp
from jax import lax
from jax.experimental import pallas as pl
from jax.experimental.pallas import tpu as pltpu
from jax.sharding import PartitionSpec as P

CORES = 2
NY = 4
SAMPLES_MOST = 128
LOW = -3.0e38
TOP = 32767.0
BOUND = 2.0e-4


def kernel(nx, nz, chunks, exact, hid, w, tgt, seg, msk, outside, o_tok, o_samp, o_bad, *scratch):
    (
        feats, weights, meta_out, meta, sent, got, logits, passing, steps_out, steps_in, errors,
        st1_out, st1, st2_out, st2, st3_out, st3,
        loc_sem, w_send, w_recv, own_send, own_recv, meta_send, meta_recv,
        xn_send, xn_recv, xf_send, xf_recv, xg_send, xg_recv,
        yo_send, yo_recv, yf_send, yf_recv, dd_send, dd_recv,
        ring_send, ring_recv, step_send, step_recv,
        s1_send, s1_recv, s2_send, s2_recv, s3_send, s3_recv, hello,
    ) = scratch
    dp = lax.axis_index("dp")
    vocab = lax.axis_index("vocab")
    x, c = dp // CORES, dp % CORES
    z, y = vocab // NY, vocab % NY
    rows = hid.shape[0]
    depth = w.shape[0]
    chip_feats = CORES * depth
    piece = chip_feats // NY
    width = weights.shape[2]
    half_cols = w.shape[1] // CORES

    def dev(xx, cc, zz, yy):
        return (xx * CORES + cc, zz * NY + yy)

    def remote(src, dst, send, recv, to):
        return pltpu.make_async_remote_copy(
            src_ref=src, dst_ref=dst, send_sem=send, recv_sem=recv,
            device_id=to, device_id_type=pl.DeviceIdType.MESH,
        )

    partner = dev(x, 1 - c, z, y)
    y_up, y_down = dev(x, c, z, (y + 1) % NY), dev(x, c, z, (y + NY - 1) % NY)
    x_up, x_down = dev((x + 1) % nx, c, z, y), dev((x + nx - 1) % nx, c, z, y)
    z_up, z_down = dev(x, c, (z + 1) % nz, y), dev(x, c, (z + nz - 1) % nz, y)
    slot1 = y * CORES + c
    n1 = NY * CORES

    def peer1(j):
        s = (slot1 + j) % n1
        return s, dev(x, s % CORES, z, s // CORES)

    def peer2(j):
        s = (z + j) % nz
        return s, dev(x, c, s, y)

    def peer3(j):
        s = (x + j) % nx
        return s, dev(s, c, z, y)

    my_rows = pl.ds(pl.multiple_of(c * rows, rows), rows)
    his_rows = pl.ds(pl.multiple_of((1 - c) * rows, rows), rows)

    meta_out[...] = jnp.zeros_like(meta_out)
    meta_out[0:1, :] = tgt[...]
    meta_out[1:2, :] = seg[...]
    meta_out[2:3, :] = msk[...]
    meta[c] = meta_out[...]
    own_cols = pl.ds(pl.multiple_of(x * chip_feats, 128), chip_feats)
    local_h = pltpu.make_async_copy(
        hid.at[:, own_cols], feats.at[x, my_rows, :], loc_sem.at[0]
    )
    local_h.start()
    my_depth = pl.ds(pl.multiple_of(c * depth, depth), depth)
    his_depth = pl.ds(pl.multiple_of((1 - c) * depth, depth), depth)
    local_w = []
    for j in range(2 * chunks):
        cols = pl.ds(pl.multiple_of(c * half_cols + j * width, 128), width)
        copy = pltpu.make_async_copy(w.at[:, cols], weights.at[j, my_depth, :], loc_sem.at[1 + j])
        copy.start()
        local_w.append(copy)

    barrier = pltpu.get_barrier_semaphore()
    def signal(sem, to):
        pl.semaphore_signal(sem, inc=1, device_id=to, device_id_type=pl.DeviceIdType.MESH)

    near = [partner, x_up, x_down, y_up, y_down, z_up, z_down]
    for p in near:
        signal(barrier, p)
    pl.semaphore_wait(barrier, len(near))

    def greet(r):
        signal(hello.at[r, 0], z_up)
        signal(hello.at[r, 1], z_down)

    def greeted(r):
        for side in range(2):
            pl.semaphore_wait(hello.at[r, side], 1)

    greet(0)
    half = rows // 2
    sides = (0, 1)
    x_to, y_to = (x_up, x_down), (y_up, y_down)
    up, down, far = (x + 1) % nx, (x + nx - 1) % nx, (x + 2) % nx
    source = (down, up, far)
    y_cols = pl.ds(pl.multiple_of(y * piece, 128), piece)

    def spot(s, which, h):
        at = pl.ds(pl.multiple_of(c * rows + h * half, half), half)
        cols = pl.ds(pl.multiple_of(((y + which) % NY) * piece, 128), piece)
        return feats.at[s, at, cols]

    def mine(to, h):
        cols = pl.ds(pl.multiple_of(to * chip_feats + y * piece, 128), piece)
        return hid.at[pl.ds(h * half, half), cols]

    def x_near(side, h):
        return remote(
            mine((up, down)[side], h), spot(x, 0, h), xn_send.at[side, h], xn_recv.at[side, h], x_to[side]
        )

    def x_far(side):
        return remote(mine(far, side), passing.at[side], xf_send.at[side], xf_recv.at[side], x_to[side])

    def x_pass(side):
        return remote(
            passing.at[side], spot(source[side], 0, side), xg_send.at[side], xg_recv.at[side], x_to[side]
        )

    def w_copy(j):
        cols = pl.ds(pl.multiple_of((1 - c) * half_cols + j * width, 128), width)
        return remote(w.at[:, cols], weights.at[j, my_depth, :], w_send.at[j], w_recv.at[j], partner)

    def y_own(q, h, side):
        ref = spot(source[q], 0, h)
        return remote(ref, ref, yo_send.at[q, h, side], yo_recv.at[q, h, side], y_to[side])

    def y_pass(q, side):
        ref = spot(source[q], (NY - 1, 1)[side], side)
        return remote(ref, ref, yf_send.at[q, side], yf_recv.at[q, side], y_to[side])

    def across(q, which, h):
        ref = spot(source[q], which, h)
        return remote(ref, ref, dd_send.at[q, which, h], dd_recv.at[q, which, h], partner)

    def landed(ref, send, recv):
        remote(ref, ref, send, recv, partner).wait_recv()

    def begin(q, h):
        for side in sides:
            y_own(q, h, side).start()
        across(q, 0, h).start()

    def middle(q, h):
        for side in sides:
            landed(spot(source[q], (NY - 1, 1)[side], h), yo_send.at[q, h, side], yo_recv.at[q, h, side])
            if side == h:
                y_pass(q, side).start()
            across(q, (NY - 1, 1)[side], h).start()

    def finish(q):
        for side in sides:
            landed(spot(source[q], 2, side), yf_send.at[q, side], yf_recv.at[q, side])
            across(q, 2, side).start()

    def whole(q):
        for which in range(NY):
            for h in sides:
                ref = feats.at[
                    source[q],
                    pl.ds(pl.multiple_of((1 - c) * rows + h * half, half), half),
                    pl.ds(pl.multiple_of(((y + which) % NY) * piece, 128), piece),
                ]
                landed(ref, dd_send.at[q, which, h], dd_recv.at[q, which, h])

    for h in sides:
        for side in sides:
            x_near(side, h).start()
    for side in sides:
        x_far(side).start()
    w_order = [i * chunks + k for k in range(chunks) for i in range(2)]
    for j in w_order:
        w_copy(j).start()
    own_copy = remote(hid.at[:, own_cols], feats.at[x, my_rows, :], own_send, own_recv, partner)
    own_copy.start()
    meta_copy = remote(meta_out, meta.at[c], meta_send, meta_recv, partner)
    meta_copy.start()
    greeted(0)
    greet(1)

    for h in sides:
        for q in sides:
            landed(spot(source[q], 0, h), xn_send.at[q, h], xn_recv.at[q, h])
            begin(q, h)
    for side in sides:
        x_far(side).wait_recv()
        x_pass(side).start()
    greeted(1)
    greet(2)
    for h in sides:
        for q in sides:
            middle(q, h)
    for side in sides:
        landed(spot(far, 0, side), xg_send.at[side], xg_recv.at[side])
        begin(2, side)
    for q in sides:
        finish(q)
    for q in sides:
        whole(q)
    for copy in local_w:
        copy.wait()
    for j in range(2 * chunks):
        w_copy(j).wait_recv()
    greeted(2)

    def part(block, j):
        return jnp.dot(feats[block], weights[j], preferred_element_type=jnp.float32)

    targets = (x_down, x_up, x_up, x_down, x_down, x_up)

    def message(i, k):
        return remote(sent.at[i, k], got.at[i, k], ring_send.at[i, k], ring_recv.at[i, k], targets[i])

    def message_steps(i, k):
        return remote(
            steps_out.at[i, k], steps_in.at[i, k], step_send.at[i, k], step_recv.at[i, k], targets[i]
        )

    def put(i, k, value, error=None):
        if exact:
            sent[i, k] = value
            message(i, k).start()
            return
        peak = jnp.max(jnp.abs(value), axis=0, keepdims=True)
        step = jnp.maximum(peak, 1.0e-30) * (1.0 / TOP)
        sent[i, k] = jnp.round(value * (1.0 / step)).astype(jnp.int32).astype(jnp.int16)
        own_error = step * 0.51
        steps_out[i, k] = jnp.concatenate([step, own_error if error is None else own_error + error], axis=0)
        message(i, k).start()
        message_steps(i, k).start()

    def take(i, k):
        message(i, k).wait_recv()
        if exact:
            return got[i, k], None
        message_steps(i, k).wait_recv()
        both = steps_in[i, k]
        return got[i, k].astype(jnp.int32).astype(jnp.float32) * both[0:1], both[1:2]

    def direct(k, carry):
        put(2, k, part(up, k))
        put(3, k, part(down, chunks + k))
        return carry

    lax.fori_loop(0, chunks, direct, 0)
    for h in sides:
        middle(2, h)
    finish(2)
    whole(2)

    def first(k, carry):
        put(0, k, part(far, k))
        put(1, k, part(far, chunks + k))
        return carry

    lax.fori_loop(0, chunks, first, 0)

    def relay(k, carry):
        for i, block in ((0, down), (1, up)):
            mine_too = part(block, i * chunks + k)
            value, error = take(i, k)
            put(4 + i, k, mine_too + value, error)
        return carry

    lax.fori_loop(0, chunks, relay, 0)

    local_h.wait()
    own_copy.wait_recv()
    meta_copy.wait_recv()

    def own(k, carry):
        for i in range(2):
            mine_too = part(x, i * chunks + k)
            value, error = take(2 + i, k)
            logits[i * chunks + k] = mine_too + value
            if not exact:
                errors[i * chunks + k] = error
        return carry

    lax.fori_loop(0, chunks, own, 0)

    eye = lax.broadcasted_iota(jnp.int32, (rows, rows), 0) == lax.broadcasted_iota(jnp.int32, (rows, rows), 1)

    def to_column(row):
        return jnp.sum(jnp.where(eye, jnp.broadcast_to(row, (rows, rows)), 0.0), axis=1, keepdims=True)

    def to_row(column):
        return jnp.sum(jnp.where(eye, jnp.broadcast_to(column, (rows, rows)), 0.0), axis=0, keepdims=True)

    base = vocab * w.shape[1] + c * half_cols
    target_column = jnp.concatenate(
        [to_column((meta[i, 0:1, :] - base).astype(jnp.float32)) for i in range(CORES)], axis=0
    ).astype(jnp.int32)
    lane = lax.broadcasted_iota(jnp.int32, (CORES * rows, width), 1)

    def stats(j, value, carry):
        largest, total, picked = carry
        new = jnp.maximum(largest, jnp.max(value, axis=1, keepdims=True))
        total = total * jnp.exp(largest - new) + jnp.sum(jnp.exp(value - new), axis=1, keepdims=True)
        hit = lane == target_column - j * width
        picked = picked + jnp.sum(jnp.where(hit, value, 0.0), axis=1, keepdims=True)
        return new, total, picked

    def last(k, carry):
        found, worst = carry
        for i in range(2):
            j = i * chunks + k
            value, error = take(4 + i, k)
            found = stats(j, logits[j] + value, found)
            if not exact:
                worst = jnp.maximum(worst, errors[j] + error)
        return found, worst

    column = (CORES * rows, 1)
    zero = jnp.zeros(column, jnp.float32)
    start = (jnp.full(column, LOW, jnp.float32), zero, zero), jnp.zeros((1, width), jnp.float32)
    found, worst = lax.fori_loop(0, chunks, last, start)

    for kind, value in enumerate(found):
        for i in range(CORES):
            st1_out[2 * kind + i : 2 * kind + i + 1, :] = to_row(value[i * rows : (i + 1) * rows])
    st1_out[6:8, :] = jnp.broadcast_to(jnp.max(worst, axis=1, keepdims=True), (2, rows))

    def exchange(n, me, peer, out, buf, send, recv):
        buf[me] = out[...]
        copies = []
        for j in range(1, n):
            _, to = peer(j)
            copy = remote(out, buf.at[me], send.at[j], recv.at[me], to)
            copy.start()
            copies.append(copy)
        for j in range(1, n):
            s, to = peer(j)
            remote(out, buf.at[s], send.at[j], recv.at[s], to).wait_recv()
        return copies

    def merged(n, buf):
        largest = buf[0, 0:2, :]
        for i in range(1, n):
            largest = jnp.maximum(largest, buf[i, 0:2, :])
        total, picked = jnp.zeros_like(largest), jnp.zeros_like(largest)
        for i in range(n):
            total = total + buf[i, 2:4, :] * jnp.exp(buf[i, 0:2, :] - largest)
            picked = picked + buf[i, 4:6, :]
        worst = buf[0, 6:8, :]
        for i in range(1, n):
            worst = jnp.maximum(worst, buf[i, 6:8, :])
        return largest, total, picked, worst

    pending = exchange(n1, slot1, peer1, st1_out, st1, s1_send, s1_recv)
    for kind, value in enumerate(merged(n1, st1)):
        st2_out[2 * kind : 2 * kind + 2, :] = value
    pending += exchange(nz, z, peer2, st2_out, st2, s2_send, s2_recv)
    largest, total, picked, worst = merged(nz, st2)
    loss = largest + jnp.log(total) - picked
    o_tok[...] = jnp.where(c == 0, loss[0:1], loss[1:2])

    ids = lax.broadcasted_iota(jnp.int32, (SAMPLES_MOST, rows), 0)
    sums, counts = jnp.zeros((SAMPLES_MOST, 1), jnp.float32), jnp.zeros((SAMPLES_MOST, 1), jnp.float32)
    for i in range(CORES):
        member = ids == meta[i, 1:2, :]
        weight = meta[i, 2:3, :].astype(jnp.float32)
        sums = sums + jnp.sum(jnp.where(member, weight * loss[i : i + 1], 0.0), axis=1, keepdims=True)
        counts = counts + jnp.sum(jnp.where(member, weight, 0.0), axis=1, keepdims=True)
    st3_out[...] = jnp.zeros_like(st3_out)
    st3_out[0:1, :] = to_row(sums)
    st3_out[1:2, :] = to_row(counts)
    norm = jnp.sum(loss * loss, axis=1, keepdims=True)
    limit = rows * (2.0 * worst[:, 0:1]) ** 2
    bad = jnp.max(jnp.where(limit <= BOUND**2 * norm, 0.0, 1.0), axis=0, keepdims=True)
    st3_out[2:3, :] = jnp.broadcast_to(bad, (1, SAMPLES_MOST))
    st3_out[3:4, :] = worst[0:1]
    pending += exchange(nx, x, peer3, st3_out, st3, s3_send, s3_recv)
    everything, most = st3[0], st3[0]
    for i in range(1, nx):
        everything = everything + st3[i]
        most = jnp.maximum(most, st3[i])
    samples = outside.shape[1]
    count = everything[1:2, :samples]
    denom = jnp.maximum(count + outside[...].astype(jnp.float32), 1.0)
    sample_loss = everything[0:1, :samples] / denom
    o_samp[...] = sample_loss
    off = 2.0 * most[3:4, :samples] * count / denom
    fine = jnp.sum(off * off, axis=1, keepdims=True) <= BOUND**2 * jnp.sum(
        sample_loss * sample_loss, axis=1, keepdims=True
    )
    o_bad[...] = jnp.maximum(most[2:3, :], jnp.where(fine, 0.0, 1.0))

    for copy in pending:
        copy.wait_send()
    for side in sides:
        x_far(side).wait_send()
        x_pass(side).wait_send()
        for h in sides:
            x_near(side, h).wait_send()
    for q in range(3):
        for side in sides:
            y_pass(q, side).wait_send()
            for h in sides:
                y_own(q, h, side).wait_send()
        for which in range(NY):
            for h in sides:
                across(q, which, h).wait_send()
    for j in range(2 * chunks):
        w_copy(j).wait_send()
    own_copy.wait_send()
    meta_copy.wait_send()

    def drain(k, carry):
        for i in range(6):
            message(i, k).wait_send()
            if not exact:
                message_steps(i, k).wait_send()
        return carry

    lax.fori_loop(0, chunks, drain, 0)


def run(nx, nz, exact, hidden, out_weight, targets, segment, loss_mask, outside_count):
    rows, depth = hidden.shape[0], out_weight.shape[0]
    half_cols = out_weight.shape[1] // CORES
    width = min(256, half_cols // 2)
    chunks = half_cols // 2 // width
    f32, dma = jnp.float32, pltpu.SemaphoreType.DMA
    coded = f32 if exact else jnp.int16
    samples = outside_count.shape[0]
    n1 = NY * CORES
    vmem = pl.BlockSpec(memory_space=pltpu.VMEM)
    anywhere = pl.BlockSpec(memory_space=pl.ANY)
    pairs = []
    for shape in [(2, 2), (2,), (2,), (3, 2, 2), (3, 2), (3, NY, 2), (6, chunks), (6, chunks), (n1,), (nz,), (nx,)]:
        pairs += [dma(shape), dma(shape)]
    return pl.pallas_call(
        functools.partial(kernel, nx, nz, chunks, exact),
        out_shape=(
            jax.ShapeDtypeStruct((1, rows), f32),
            jax.ShapeDtypeStruct((1, samples), f32),
            jax.ShapeDtypeStruct((1, SAMPLES_MOST), f32),
        ),
        in_specs=[anywhere, anywhere, vmem, vmem, vmem, vmem],
        out_specs=(vmem, vmem, vmem),
        scratch_shapes=[
            pltpu.VMEM((nx, CORES * rows, CORES * depth), jnp.bfloat16),
            pltpu.VMEM((2 * chunks, CORES * depth, width), jnp.bfloat16),
            pltpu.VMEM((8, rows), jnp.int32),
            pltpu.VMEM((CORES, 8, rows), jnp.int32),
            pltpu.VMEM((6, chunks, CORES * rows, width), coded),
            pltpu.VMEM((6, chunks, CORES * rows, width), coded),
            pltpu.VMEM((2 * chunks, CORES * rows, width), f32),
            pltpu.VMEM((2, rows // 2, CORES * depth // NY), jnp.bfloat16),
            pltpu.VMEM((6, chunks, 2, width), f32),
            pltpu.VMEM((6, chunks, 2, width), f32),
            pltpu.VMEM((2 * chunks, 1, width), f32),
            pltpu.VMEM((8, rows), f32),
            pltpu.VMEM((n1, 8, rows), f32),
            pltpu.VMEM((8, rows), f32),
            pltpu.VMEM((nz, 8, rows), f32),
            pltpu.VMEM((8, SAMPLES_MOST), f32),
            pltpu.VMEM((nx, 8, SAMPLES_MOST), f32),
            dma((1 + 2 * chunks,)),
            dma((2 * chunks,)), dma((2 * chunks,)),
            dma, dma, dma, dma,
            *pairs,
            pltpu.SemaphoreType.REGULAR((3, 2)),
        ],
        compiler_params=pltpu.CompilerParams(collective_id=int(exact), has_side_effects=True),
    )(
        hidden, out_weight, targets[None], segment[None], loss_mask[None], outside_count[None]
    )


def body(nx, nz, *arrays):
    tok, samp, bad = run(nx, nz, False, *arrays)
    tok, samp = lax.cond(
        bad[0, 0] > 0.0,
        lambda *_: run(nx, nz, True, *arrays)[:2],
        lambda *found: found,
        tok, samp,
    )
    return tok.reshape(-1), samp.reshape(-1)


def solution(mesh):
    nx = mesh.shape["dp"] // CORES
    nz = mesh.shape["vocab"] // NY
    return jax.shard_map(
        functools.partial(body, nx, nz),
        mesh=mesh,
        in_specs=(P("dp", None), P("dp", "vocab"), P("dp"), P("dp"), P("dp"), P()),
        out_specs=(P("dp"), P()),
        check_vma=False,
    )
```

```python
import functools

import jax
import jax.numpy as jnp
from jax import lax
from jax.experimental import pallas as pl
from jax.experimental.pallas import tpu as pltpu
from jax.sharding import PartitionSpec as P

CORES = 2
NY = 4
SAMPLES_MOST = 128
LOW = -3.0e38
TOP = 32767.0
BOUND = 2.0e-4


def kernel(nx, nz, chunks, exact, hid, w, tgt, seg, msk, outside, o_tok, o_samp, o_bad, *scratch):
    (
        feats, weights, meta_out, meta, sent, got, logits, passing, steps_out, steps_in, errors,
        st1_out, st1, st2_out, st2, st3_out, st3,
        loc_sem, w_send, w_recv, own_send, own_recv, meta_send, meta_recv,
        xn_send, xn_recv, xf_send, xf_recv, xg_send, xg_recv,
        yo_send, yo_recv, yf_send, yf_recv, dd_send, dd_recv,
        ring_send, ring_recv, step_send, step_recv,
        s1_send, s1_recv, s2_send, s2_recv, s3_send, s3_recv, hello,
    ) = scratch
    dp = lax.axis_index("dp")
    vocab = lax.axis_index("vocab")
    x, c = dp // CORES, dp % CORES
    z, y = vocab // NY, vocab % NY
    rows = hid.shape[0]
    depth = w.shape[0]
    chip_feats = CORES * depth
    piece = chip_feats // NY
    width = weights.shape[2]
    half_cols = w.shape[1] // CORES

    def dev(xx, cc, zz, yy):
        return (xx * CORES + cc, zz * NY + yy)

    def remote(src, dst, send, recv, to):
        return pltpu.make_async_remote_copy(
            src_ref=src, dst_ref=dst, send_sem=send, recv_sem=recv,
            device_id=to, device_id_type=pl.DeviceIdType.MESH,
        )

    partner = dev(x, 1 - c, z, y)
    y_up, y_down = dev(x, c, z, (y + 1) % NY), dev(x, c, z, (y + NY - 1) % NY)
    x_up, x_down = dev((x + 1) % nx, c, z, y), dev((x + nx - 1) % nx, c, z, y)
    z_up, z_down = dev(x, c, (z + 1) % nz, y), dev(x, c, (z + nz - 1) % nz, y)
    slot1 = y * CORES + c
    n1 = NY * CORES

    def peer1(j):
        s = (slot1 + j) % n1
        return s, dev(x, s % CORES, z, s // CORES)

    def peer2(j):
        s = (z + j) % nz
        return s, dev(x, c, s, y)

    def peer3(j):
        s = (x + j) % nx
        return s, dev(s, c, z, y)

    my_rows = pl.ds(pl.multiple_of(c * rows, rows), rows)
    his_rows = pl.ds(pl.multiple_of((1 - c) * rows, rows), rows)

    meta_out[...] = jnp.zeros_like(meta_out)
    meta_out[0:1, :] = tgt[...]
    meta_out[1:2, :] = seg[...]
    meta_out[2:3, :] = msk[...]
    meta[c] = meta_out[...]
    own_cols = pl.ds(pl.multiple_of(x * chip_feats, 128), chip_feats)
    local_h = pltpu.make_async_copy(
        hid.at[:, own_cols], feats.at[x, my_rows, :], loc_sem.at[0]
    )
    local_h.start()
    my_depth = pl.ds(pl.multiple_of(c * depth, depth), depth)
    his_depth = pl.ds(pl.multiple_of((1 - c) * depth, depth), depth)
    local_w = []
    for j in range(2 * chunks):
        cols = pl.ds(pl.multiple_of(c * half_cols + j * width, 128), width)
        copy = pltpu.make_async_copy(w.at[:, cols], weights.at[j, my_depth, :], loc_sem.at[1 + j])
        copy.start()
        local_w.append(copy)

    barrier = pltpu.get_barrier_semaphore()
    def signal(sem, to):
        pl.semaphore_signal(sem, inc=1, device_id=to, device_id_type=pl.DeviceIdType.MESH)

    near = [partner, x_up, x_down, y_up, y_down, z_up, z_down]
    for p in near:
        signal(barrier, p)
    pl.semaphore_wait(barrier, len(near))

    def greet(r):
        signal(hello.at[r, 0], z_up)
        signal(hello.at[r, 1], z_down)

    def greeted(r):
        for side in range(2):
            pl.semaphore_wait(hello.at[r, side], 1)

    greet(0)
    half = rows // 2
    sides = (0, 1)
    x_to, y_to, z_to = (x_up, x_down), (y_up, y_down), (z_up, z_down)
    up, down, far = (x + 1) % nx, (x + nx - 1) % nx, (x + 2) % nx
    source = (down, up, far)
    label = ((y + 2 * z) % NY, (z + 2 * y) % NY, (y + 2 * z) % NY)
    beside = (y_to, z_to, y_to)
    across_to = (z_to, y_to, z_to)

    def spot(s, q, which, h):
        at = pl.ds(pl.multiple_of(c * rows + h * half, half), half)
        cols = pl.ds(pl.multiple_of(((label[q] + which) % NY) * piece, 128), piece)
        return feats.at[s, at, cols]

    def mine(to, q, h):
        cols = pl.ds(pl.multiple_of(to * chip_feats + label[q] * piece, 128), piece)
        return hid.at[pl.ds(h * half, half), cols]

    def x_near(side, h):
        return remote(
            mine((up, down)[side], side, h), spot(x, side, 0, h),
            xn_send.at[side, h], xn_recv.at[side, h], x_to[side],
        )

    def x_far(side):
        return remote(mine(far, 2, side), passing.at[side], xf_send.at[side], xf_recv.at[side], x_to[side])

    def x_pass(side):
        return remote(
            passing.at[side], spot(source[side], 2, 0, side), xg_send.at[side], xg_recv.at[side], x_to[side]
        )

    def w_copy(j):
        cols = pl.ds(pl.multiple_of((1 - c) * half_cols + j * width, 128), width)
        return remote(w.at[:, cols], weights.at[j, my_depth, :], w_send.at[j], w_recv.at[j], partner)

    def one(q, h, side):
        ref = spot(source[q], q, 0, h)
        return remote(ref, ref, yo_send.at[q, h, side], yo_recv.at[q, h, side], beside[q][side])

    def two(q, side):
        ref = spot(source[q], q, 0, side)
        return remote(ref, ref, yf_send.at[q, side], yf_recv.at[q, side], across_to[q][side])

    def across(q, which, h):
        ref = spot(source[q], q, which, h)
        return remote(ref, ref, dd_send.at[q, which, h], dd_recv.at[q, which, h], partner)

    def landed(ref, send, recv):
        remote(ref, ref, send, recv, partner).wait_recv()

    def begin(q, h):
        for side in sides:
            one(q, h, side).start()
        two(q, h).start()
        across(q, 0, h).start()

    def middle(q, h):
        for side in sides:
            which = (NY - 1, 1)[side]
            landed(spot(source[q], q, which, h), yo_send.at[q, h, side], yo_recv.at[q, h, side])
            across(q, which, h).start()
        landed(spot(source[q], q, 2, h), yf_send.at[q, h], yf_recv.at[q, h])
        across(q, 2, h).start()

    def whole(q):
        for which in range(NY):
            for h in sides:
                ref = feats.at[
                    source[q],
                    pl.ds(pl.multiple_of((1 - c) * rows + h * half, half), half),
                    pl.ds(pl.multiple_of(((label[q] + which) % NY) * piece, 128), piece),
                ]
                landed(ref, dd_send.at[q, which, h], dd_recv.at[q, which, h])

    for h in sides:
        for side in sides:
            x_near(side, h).start()
    for side in sides:
        x_far(side).start()
    w_order = [i * chunks + k for k in range(chunks) for i in range(2)]
    for j in w_order:
        w_copy(j).start()
    own_copy = remote(hid.at[:, own_cols], feats.at[x, my_rows, :], own_send, own_recv, partner)
    own_copy.start()
    meta_copy = remote(meta_out, meta.at[c], meta_send, meta_recv, partner)
    meta_copy.start()
    greeted(0)
    greet(1)

    for h in sides:
        for q in sides:
            landed(spot(source[q], q, 0, h), xn_send.at[q, h], xn_recv.at[q, h])
            begin(q, h)
    for side in sides:
        x_far(side).wait_recv()
        x_pass(side).start()
    greeted(1)
    greet(2)
    for h in sides:
        for q in sides:
            middle(q, h)
    for side in sides:
        landed(spot(far, 2, 0, side), xg_send.at[side], xg_recv.at[side])
        begin(2, side)
    for q in sides:
        whole(q)
    for copy in local_w:
        copy.wait()
    for j in range(2 * chunks):
        w_copy(j).wait_recv()
    greeted(2)

    def part(block, j):
        return jnp.dot(feats[block], weights[j], preferred_element_type=jnp.float32)

    targets = (x_down, x_up, x_up, x_down, x_down, x_up)

    def message(i, k):
        return remote(sent.at[i, k], got.at[i, k], ring_send.at[i, k], ring_recv.at[i, k], targets[i])

    def message_steps(i, k):
        return remote(
            steps_out.at[i, k], steps_in.at[i, k], step_send.at[i, k], step_recv.at[i, k], targets[i]
        )

    def put(i, k, value, error=None):
        if exact:
            sent[i, k] = value
            message(i, k).start()
            return
        peak = jnp.max(jnp.abs(value), axis=0, keepdims=True)
        step = jnp.maximum(peak, 1.0e-30) * (1.0 / TOP)
        sent[i, k] = jnp.round(value * (1.0 / step)).astype(jnp.int32).astype(jnp.int16)
        own_error = step * 0.51
        steps_out[i, k] = jnp.concatenate([step, own_error if error is None else own_error + error], axis=0)
        message(i, k).start()
        message_steps(i, k).start()

    def take(i, k):
        message(i, k).wait_recv()
        if exact:
            return got[i, k], None
        message_steps(i, k).wait_recv()
        both = steps_in[i, k]
        return got[i, k].astype(jnp.int32).astype(jnp.float32) * both[0:1], both[1:2]

    def direct(k, carry):
        put(2, k, part(up, k))
        put(3, k, part(down, chunks + k))
        return carry

    lax.fori_loop(0, chunks, direct, 0)
    for h in sides:
        middle(2, h)
    whole(2)

    def first(k, carry):
        put(0, k, part(far, k))
        put(1, k, part(far, chunks + k))
        return carry

    lax.fori_loop(0, chunks, first, 0)

    def relay(k, carry):
        for i, block in ((0, down), (1, up)):
            mine_too = part(block, i * chunks + k)
            value, error = take(i, k)
            put(4 + i, k, mine_too + value, error)
        return carry

    lax.fori_loop(0, chunks, relay, 0)

    local_h.wait()
    own_copy.wait_recv()
    meta_copy.wait_recv()

    def own(k, carry):
        for i in range(2):
            mine_too = part(x, i * chunks + k)
            value, error = take(2 + i, k)
            logits[i * chunks + k] = mine_too + value
            if not exact:
                errors[i * chunks + k] = error
        return carry

    lax.fori_loop(0, chunks, own, 0)

    eye = lax.broadcasted_iota(jnp.int32, (rows, rows), 0) == lax.broadcasted_iota(jnp.int32, (rows, rows), 1)

    def to_column(row):
        return jnp.sum(jnp.where(eye, jnp.broadcast_to(row, (rows, rows)), 0.0), axis=1, keepdims=True)

    def to_row(column):
        return jnp.sum(jnp.where(eye, jnp.broadcast_to(column, (rows, rows)), 0.0), axis=0, keepdims=True)

    base = vocab * w.shape[1] + c * half_cols
    target_column = jnp.concatenate(
        [to_column((meta[i, 0:1, :] - base).astype(jnp.float32)) for i in range(CORES)], axis=0
    ).astype(jnp.int32)
    lane = lax.broadcasted_iota(jnp.int32, (CORES * rows, width), 1)

    def stats(j, value, carry):
        largest, total, picked = carry
        new = jnp.maximum(largest, jnp.max(value, axis=1, keepdims=True))
        total = total * jnp.exp(largest - new) + jnp.sum(jnp.exp(value - new), axis=1, keepdims=True)
        hit = lane == target_column - j * width
        picked = picked + jnp.sum(jnp.where(hit, value, 0.0), axis=1, keepdims=True)
        return new, total, picked

    def last(k, carry):
        found, worst = carry
        for i in range(2):
            j = i * chunks + k
            value, error = take(4 + i, k)
            found = stats(j, logits[j] + value, found)
            if not exact:
                worst = jnp.maximum(worst, errors[j] + error)
        return found, worst

    column = (CORES * rows, 1)
    zero = jnp.zeros(column, jnp.float32)
    start = (jnp.full(column, LOW, jnp.float32), zero, zero), jnp.zeros((1, width), jnp.float32)
    found, worst = lax.fori_loop(0, chunks, last, start)

    for kind, value in enumerate(found):
        for i in range(CORES):
            st1_out[2 * kind + i : 2 * kind + i + 1, :] = to_row(value[i * rows : (i + 1) * rows])
    st1_out[6:8, :] = jnp.broadcast_to(jnp.max(worst, axis=1, keepdims=True), (2, rows))

    def exchange(n, me, peer, out, buf, send, recv):
        buf[me] = out[...]
        copies = []
        for j in range(1, n):
            _, to = peer(j)
            copy = remote(out, buf.at[me], send.at[j], recv.at[me], to)
            copy.start()
            copies.append(copy)
        for j in range(1, n):
            s, to = peer(j)
            remote(out, buf.at[s], send.at[j], recv.at[s], to).wait_recv()
        return copies

    def merged(n, buf):
        largest = buf[0, 0:2, :]
        for i in range(1, n):
            largest = jnp.maximum(largest, buf[i, 0:2, :])
        total, picked = jnp.zeros_like(largest), jnp.zeros_like(largest)
        for i in range(n):
            total = total + buf[i, 2:4, :] * jnp.exp(buf[i, 0:2, :] - largest)
            picked = picked + buf[i, 4:6, :]
        worst = buf[0, 6:8, :]
        for i in range(1, n):
            worst = jnp.maximum(worst, buf[i, 6:8, :])
        return largest, total, picked, worst

    pending = exchange(n1, slot1, peer1, st1_out, st1, s1_send, s1_recv)
    for kind, value in enumerate(merged(n1, st1)):
        st2_out[2 * kind : 2 * kind + 2, :] = value
    pending += exchange(nz, z, peer2, st2_out, st2, s2_send, s2_recv)
    largest, total, picked, worst = merged(nz, st2)
    loss = largest + jnp.log(total) - picked
    o_tok[...] = jnp.where(c == 0, loss[0:1], loss[1:2])

    ids = lax.broadcasted_iota(jnp.int32, (SAMPLES_MOST, rows), 0)
    sums, counts = jnp.zeros((SAMPLES_MOST, 1), jnp.float32), jnp.zeros((SAMPLES_MOST, 1), jnp.float32)
    for i in range(CORES):
        member = ids == meta[i, 1:2, :]
        weight = meta[i, 2:3, :].astype(jnp.float32)
        sums = sums + jnp.sum(jnp.where(member, weight * loss[i : i + 1], 0.0), axis=1, keepdims=True)
        counts = counts + jnp.sum(jnp.where(member, weight, 0.0), axis=1, keepdims=True)
    st3_out[...] = jnp.zeros_like(st3_out)
    st3_out[0:1, :] = to_row(sums)
    st3_out[1:2, :] = to_row(counts)
    norm = jnp.sum(loss * loss, axis=1, keepdims=True)
    limit = rows * (2.0 * worst[:, 0:1]) ** 2
    bad = jnp.max(jnp.where(limit <= BOUND**2 * norm, 0.0, 1.0), axis=0, keepdims=True)
    st3_out[2:3, :] = jnp.broadcast_to(bad, (1, SAMPLES_MOST))
    st3_out[3:4, :] = worst[0:1]
    pending += exchange(nx, x, peer3, st3_out, st3, s3_send, s3_recv)
    everything, most = st3[0], st3[0]
    for i in range(1, nx):
        everything = everything + st3[i]
        most = jnp.maximum(most, st3[i])
    samples = outside.shape[1]
    count = everything[1:2, :samples]
    denom = jnp.maximum(count + outside[...].astype(jnp.float32), 1.0)
    sample_loss = everything[0:1, :samples] / denom
    o_samp[...] = sample_loss
    off = 2.0 * most[3:4, :samples] * count / denom
    fine = jnp.sum(off * off, axis=1, keepdims=True) <= BOUND**2 * jnp.sum(
        sample_loss * sample_loss, axis=1, keepdims=True
    )
    o_bad[...] = jnp.maximum(most[2:3, :], jnp.where(fine, 0.0, 1.0))

    for copy in pending:
        copy.wait_send()
    for side in sides:
        x_far(side).wait_send()
        x_pass(side).wait_send()
        for h in sides:
            x_near(side, h).wait_send()
    for q in range(3):
        for side in sides:
            two(q, side).wait_send()
            for h in sides:
                one(q, h, side).wait_send()
        for which in range(NY):
            for h in sides:
                across(q, which, h).wait_send()
    for j in range(2 * chunks):
        w_copy(j).wait_send()
    own_copy.wait_send()
    meta_copy.wait_send()

    def drain(k, carry):
        for i in range(6):
            message(i, k).wait_send()
            if not exact:
                message_steps(i, k).wait_send()
        return carry

    lax.fori_loop(0, chunks, drain, 0)


def run(nx, nz, exact, hidden, out_weight, targets, segment, loss_mask, outside_count):
    rows, depth = hidden.shape[0], out_weight.shape[0]
    half_cols = out_weight.shape[1] // CORES
    width = min(256, half_cols // 2)
    chunks = half_cols // 2 // width
    f32, dma = jnp.float32, pltpu.SemaphoreType.DMA
    coded = f32 if exact else jnp.int16
    samples = outside_count.shape[0]
    n1 = NY * CORES
    vmem = pl.BlockSpec(memory_space=pltpu.VMEM)
    anywhere = pl.BlockSpec(memory_space=pl.ANY)
    pairs = []
    for shape in [(2, 2), (2,), (2,), (3, 2, 2), (3, 2), (3, NY, 2), (6, chunks), (6, chunks), (n1,), (nz,), (nx,)]:
        pairs += [dma(shape), dma(shape)]
    return pl.pallas_call(
        functools.partial(kernel, nx, nz, chunks, exact),
        out_shape=(
            jax.ShapeDtypeStruct((1, rows), f32),
            jax.ShapeDtypeStruct((1, samples), f32),
            jax.ShapeDtypeStruct((1, SAMPLES_MOST), f32),
        ),
        in_specs=[anywhere, anywhere, vmem, vmem, vmem, vmem],
        out_specs=(vmem, vmem, vmem),
        scratch_shapes=[
            pltpu.VMEM((nx, CORES * rows, CORES * depth), jnp.bfloat16),
            pltpu.VMEM((2 * chunks, CORES * depth, width), jnp.bfloat16),
            pltpu.VMEM((8, rows), jnp.int32),
            pltpu.VMEM((CORES, 8, rows), jnp.int32),
            pltpu.VMEM((6, chunks, CORES * rows, width), coded),
            pltpu.VMEM((6, chunks, CORES * rows, width), coded),
            pltpu.VMEM((2 * chunks, CORES * rows, width), f32),
            pltpu.VMEM((2, rows // 2, CORES * depth // NY), jnp.bfloat16),
            pltpu.VMEM((6, chunks, 2, width), f32),
            pltpu.VMEM((6, chunks, 2, width), f32),
            pltpu.VMEM((2 * chunks, 1, width), f32),
            pltpu.VMEM((8, rows), f32),
            pltpu.VMEM((n1, 8, rows), f32),
            pltpu.VMEM((8, rows), f32),
            pltpu.VMEM((nz, 8, rows), f32),
            pltpu.VMEM((8, SAMPLES_MOST), f32),
            pltpu.VMEM((nx, 8, SAMPLES_MOST), f32),
            dma((1 + 2 * chunks,)),
            dma((2 * chunks,)), dma((2 * chunks,)),
            dma, dma, dma, dma,
            *pairs,
            pltpu.SemaphoreType.REGULAR((3, 2)),
        ],
        compiler_params=pltpu.CompilerParams(collective_id=int(exact), has_side_effects=True),
    )(
        hidden, out_weight, targets[None], segment[None], loss_mask[None], outside_count[None]
    )


def body(nx, nz, *arrays):
    tok, samp, bad = run(nx, nz, False, *arrays)
    tok, samp = lax.cond(
        bad[0, 0] > 0.0,
        lambda *_: run(nx, nz, True, *arrays)[:2],
        lambda *found: found,
        tok, samp,
    )
    return tok.reshape(-1), samp.reshape(-1)


def solution(mesh):
    nx = mesh.shape["dp"] // CORES
    nz = mesh.shape["vocab"] // NY
    return jax.shard_map(
        functools.partial(body, nx, nz),
        mesh=mesh,
        in_specs=(P("dp", None), P("dp", "vocab"), P("dp"), P("dp"), P("dp"), P()),
        out_specs=(P("dp"), P()),
        check_vma=False,
    )
```
